256 devices in a mesh: groups: 4 (over y, x), ha: 64 (over z, core).
Axes of the slice: x: 2, y: 2, z: 32, core: 2. Of those that a mesh axis runs over, the one named last changes fastest.
The devices are a block of a 4x8x32 slice.
Arguments:
- video: bfloat16 [16, 256, 192, 192], P('groups', 'ha'), parts along dimension 0, may hold values from -6 to 6
- s1_weight: bfloat16 [3, 3, 192, 128], replicated, may hold values from -0.15625 to 0.15625
- t1_weight: bfloat16 [3, 128, 128], replicated, may hold values from -0.3125 to 0.3125
- r1_weight: bfloat16 [2, 2, 128, 256], replicated, may hold values from -0.25 to 0.25
- s2_weight: bfloat16 [3, 3, 256, 256], replicated, may hold values from -0.125 to 0.125
- t2_weight: bfloat16 [3, 256, 256], replicated, may hold values from -0.21875 to 0.21875
- r2_weight: bfloat16 [2, 2, 256, 512], replicated, may hold values from -0.1875 to 0.1875
- attn_gain: bfloat16 [512], replicated, may hold values from 0.5 to 1.5
- w_query: bfloat16 [512, 512], replicated, may hold values from -2.5 to 2.5
- w_key: bfloat16 [512, 512], replicated, may hold values from -0.27 to 0.27
- w_value: bfloat16 [512, 512], replicated, may hold values from -0.25 to 0.25
- w_out: bfloat16 [512, 512], replicated, may hold values from -1 to 1
Outputs:
- encoded: bfloat16 [16, 64, 48, 512], P('groups', 'ha'), parts along dimension 0
The draws below stay inside these ranges and needn't reach their ends.
There are 4 independent parts, one for each index of `groups`. The reference program is written for one: setup_inputs(seed, part) draws one part's arguments, and reference() takes and returns one part's arrays. A program takes and returns all parts, laid end to end along the dimension named above; an argument that names none is the same for every part. Nothing has to cross between parts.
All inputs are finite; a program needn't handle non-finite values.
Results may differ from the reference program's by a relative error of at most 0.018.
Values may be sent and summed in bfloat16 or wider, within the bound.
A program may use at most 128 MiB of HBM per device.

```python
import math
import jax
import jax.numpy as jnp
from jax import lax

C0 = 192
C1 = 128
C2 = 256
C3 = 512
FRAMES = 4
W = 192
H = 256


def key_base(key):
    raw = jax.random.truncated_normal(jax.random.fold_in(key, 71), -6.0, 6.0, (C3, C3), jnp.float32) / jnp.sqrt(jnp.float32(C3))
    return jnp.clip(raw, -0.27, 0.27)


def draw_w_key(key, part):
    return key_base(key).astype(jnp.bfloat16)


def draw_w_query(key, part):
    noise = jax.random.truncated_normal(jax.random.fold_in(key, 83), -6.0, 6.0, (C3, C3), jnp.float32) * 2.0 / jnp.sqrt(jnp.float32(C3))
    return jnp.clip(noise, -2.5, 2.5).astype(jnp.bfloat16)


def steps_of(own_key, extent, pieces, least, top_value):
    def one(axis_at, parts):
        draws = jax.random.uniform(jax.random.fold_in(jax.random.fold_in(own_key, 6), axis_at), (parts,), jnp.float32, least / len(pieces), top_value / len(pieces))
        return jnp.repeat(jnp.exp(draws), extent[axis_at] // parts).reshape((-1,) + (1,) * (len(extent) - axis_at - 1))

    factor_of = one(*pieces[0])
    for cut in pieces[1:]:
        factor_of = factor_of * one(*cut)
    return factor_of


def gaussian(own_key, extent, scale, most, shards=(), held_as=jnp.bfloat16):
    result = scale * jax.random.normal(own_key, extent, jnp.float32)
    if shards:
        result = result * steps_of(own_key, extent, shards, -0.22, 0.18)
    return jnp.clip(result, -most, most).astype(held_as)


def setup_inputs(seed: int = 0, part: int = 0) -> dict:
    streams_of = jax.random.split(jax.random.key(seed), 13)
    own_keys = jax.random.split(jax.random.fold_in(streams_of[12], part), 13)
    return {
        "video": gaussian(own_keys[0], (FRAMES, H, W, C0), 1.0, 6.0, ((1, 64),)),
        "s1_weight": gaussian(streams_of[1], (3, 3, C0, C1), (9 * C0) ** -0.5, 0.15625),
        "t1_weight": gaussian(streams_of[2], (3, C1, C1), (3 * C1) ** -0.5, 0.3125),
        "r1_weight": gaussian(streams_of[3], (2, 2, C1, C2), (4 * C1) ** -0.5, 0.25),
        "s2_weight": gaussian(streams_of[4], (3, 3, C2, C2), (9 * C2) ** -0.5, 0.125),
        "t2_weight": gaussian(streams_of[5], (3, C2, C2), (3 * C2) ** -0.5, 0.21875),
        "r2_weight": gaussian(streams_of[6], (2, 2, C2, C3), (4 * C2) ** -0.5, 0.1875),
        "attn_gain": jnp.clip(1.0 + 0.1 * jax.random.normal(streams_of[7], (C3,), jnp.float32), 0.5, 1.5).astype(jnp.bfloat16),
        "w_query": draw_w_query(jax.random.fold_in(streams_of[12], 71), part),
        "w_key": draw_w_key(jax.random.fold_in(streams_of[12], 71), part),
        "w_value": gaussian(streams_of[10], (C3, C3), C3 ** -0.5, 0.25),
        "w_out": gaussian(streams_of[11], (C3, C3), (C3 // 16) ** -0.5, 1.0),
    }


def spatial(volume, weight):
    row_count = volume.shape[1]
    col_count = volume.shape[2]
    padded = jnp.pad(volume.astype(jnp.float32), ((0, 0), (1, 1), (1, 1), (0, 0)))
    kernel = weight.astype(jnp.float32)
    summed = None
    for tap_row in range(3):
        for tap_col in range(3):
            tap_term = jnp.einsum('tywc,co->tywo', padded[:, tap_row:tap_row + row_count, tap_col:tap_col + col_count], kernel[tap_row, tap_col], precision=lax.Precision.HIGHEST)
            summed = tap_term if summed is None else summed + tap_term
    return summed

def temporal(volume, weight):
    frame_count = volume.shape[0]
    padded = jnp.pad(volume.astype(jnp.float32), ((2, 0), (0, 0), (0, 0), (0, 0)))
    kernel = weight.astype(jnp.float32)
    summed = None
    for tap_time in range(3):
        tap_term = jnp.einsum('tywc,co->tywo', padded[tap_time:tap_time + frame_count], kernel[tap_time], precision=lax.Precision.HIGHEST)
        summed = tap_term if summed is None else summed + tap_term
    return summed

def reduce_pairs(volume, weight):
    frame_count, row_count, col_count, channels = volume.shape
    grouped = volume.astype(jnp.float32).reshape(frame_count, row_count // 2, 2, col_count // 2, 2, channels)
    return jnp.einsum('tyixjc,ijco->tyxo', grouped, weight.astype(jnp.float32), precision=lax.Precision.HIGHEST)

def reference(video, s1_weight, t1_weight, r1_weight, s2_weight, t2_weight, r2_weight, attn_gain, w_query, w_key, w_value, w_out):
    a_first = spatial(video, s1_weight).astype(jnp.bfloat16)
    h_first = jax.nn.silu(temporal(a_first, t1_weight)).astype(jnp.bfloat16)
    d_first = reduce_pairs(h_first, r1_weight).astype(jnp.bfloat16)
    a_second = spatial(d_first, s2_weight).astype(jnp.bfloat16)
    h_second = (d_first.astype(jnp.float32) + jax.nn.silu(temporal(a_second, t2_weight))).astype(jnp.bfloat16)
    h_third = reduce_pairs(h_second, r2_weight).astype(jnp.bfloat16)
    frame_count, row_count, col_count, channels = h_third.shape
    flat = h_third.reshape(frame_count, row_count * col_count, channels)
    score_scale = 1.0 / math.sqrt(channels)

    def attend(sites):
        residual = sites.astype(jnp.float32)
        mean_square = lax.optimization_barrier(jnp.mean(residual * residual, axis=-1, keepdims=True))
        inverse_norm = lax.rsqrt(mean_square + 1e-06)
        normed = (residual * inverse_norm * attn_gain.astype(jnp.float32)).astype(jnp.bfloat16)
        queries = jnp.dot(normed, w_query, preferred_element_type=jnp.float32).astype(jnp.bfloat16)
        key_rows = jnp.dot(normed, w_key, preferred_element_type=jnp.float32).astype(jnp.bfloat16)
        value_rows = jnp.dot(normed, w_value, preferred_element_type=jnp.float32).astype(jnp.bfloat16)
        scores = jnp.dot(queries, key_rows.T, preferred_element_type=jnp.float32) * score_scale
        top_score = lax.optimization_barrier(jnp.max(scores, axis=-1, keepdims=True))
        weights = jnp.exp(scores - top_score)
        totals = lax.optimization_barrier(jnp.sum(weights, axis=-1, keepdims=True))
        attended = (jnp.dot(weights.astype(jnp.bfloat16), value_rows, preferred_element_type=jnp.float32) / totals).astype(jnp.bfloat16)
        return (residual + jnp.dot(attended, w_out, preferred_element_type=jnp.float32)).astype(jnp.bfloat16)
    encoded = lax.map(attend, flat)
    return encoded.reshape(frame_count, row_count, col_count, channels)
```

```python
import functools
import math

import jax
import jax.numpy as jnp
from jax import lax
from jax.experimental import pallas as pl
from jax.experimental.pallas import tpu as pltpu
from jax.sharding import PartitionSpec as P

F32 = jnp.float32
BF16 = jnp.bfloat16


def silu(x):
    return x / (1.0 + jnp.exp(-x))


def side_sum(acc, width, period):
    rows = acc.shape[0]
    site = lax.rem(lax.broadcasted_iota(jnp.int32, (rows, width), 0), period)
    low = pltpu.roll(acc[:, :width], 1, 0)
    high = pltpu.roll(acc[:, 2 * width :], rows - 1, 0)
    low = jnp.where(site == 0, 0.0, low)
    high = jnp.where(site == period - 1, 0.0, high)
    return acc[:, width : 2 * width] + low + high


def kernel(
    n,
    video,
    s1,
    t1,
    r1,
    s2,
    t2,
    r2,
    gain,
    wq,
    wk,
    wv,
    wo,
    out,
    vp,
    w1,
    t1v,
    r1v,
    w2,
    t2v,
    r2v,
    gainv,
    wqv,
    wkv,
    wvv,
    wov,
    a1p,
    h1s,
    d1p,
    a2p,
    h2s,
    res,
    keys,
    qp,
    top,
    total,
    mixed,
    video_sem,
    w1_sem,
    w2_sem,
    weight_sem,
    halo1_send,
    halo1_recv,
    halo2_send,
    halo2_recv,
    own_send,
    own_recv,
    ring_send,
    ring_recv,
    pair_send,
    pair_recv,
    last_send,
):
    frames, rows, width, _ = video.shape
    c1 = t1.shape[1]
    c2 = t2.shape[1]
    c3 = wq.shape[0]
    half_rows, half_width = rows // 2, width // 2
    sites = out.shape[1] * out.shape[2]
    half = frames // 2
    hops = n // 4

    ha = lax.axis_index("ha")
    core = lax.rem(ha, 2)
    up = lax.rem(ha + n - 1, n)
    down = lax.rem(ha + 1, n)
    partner = ha + 1 - 2 * core
    after = lax.rem(ha + n + 2 - 4 * core, n)
    two_up = lax.rem(ha + n - 2, n)
    two_down = lax.rem(ha + 2, n)

    def video_copy(t):
        return pltpu.make_async_copy(video.at[t], vp.at[t, pl.ds(1, rows)], video_sem.at[t])

    def w1_copy(i, j):
        return pltpu.make_async_copy(
            s1.at[i, j], w1.at[i, :, pl.ds(j * c1, c1)], w1_sem.at[i, j]
        )

    def w2_copy(i, j):
        return pltpu.make_async_copy(
            s2.at[i, j], w2.at[i, :, pl.ds(j * c2, c2)], w2_sem.at[i, j]
        )

    plain = ((t1, t1v), (r1, r1v), (t2, t2v), (r2, r2v), (gain, gainv), (wq, wqv), (wk, wkv), (wv, wvv), (wo, wov))

    def plain_copy(k):
        return pltpu.make_async_copy(plain[k][0], plain[k][1], weight_sem.at[k])

    for i in range(3):
        for j in range(3):
            w1_copy(i, j).start()
    for t in range(frames):
        video_copy(t).start()
    for k in range(2):
        plain_copy(k).start()

    barrier = pltpu.get_barrier_semaphore()
    for other in (up, down, two_up, two_down):
        pl.semaphore_signal(
            barrier, inc=1, device_id={"ha": other}, device_id_type=pl.DeviceIdType.MESH
        )
    pl.semaphore_wait(barrier, 4)

    def remote(src, dst, send, recv, to):
        return pltpu.make_async_remote_copy(
            src_ref=src,
            dst_ref=dst,
            send_sem=send,
            recv_sem=recv,
            device_id={"ha": to},
            device_id_type=pl.DeviceIdType.MESH,
        )

    def halo1(d, t):
        if d == 0:
            src, dst, to = video.at[t, rows - 1], vp.at[t, 0], down
        else:
            src, dst, to = video.at[t, 0], vp.at[t, rows + 1], up
        return remote(src, dst, halo1_send.at[d, t], halo1_recv.at[d, t], to)

    def halo2(d, t):
        if d == 0:
            src, dst, to = d1p.at[t, half_rows], d1p.at[t, 0], down
        else:
            src, dst, to = d1p.at[t, 1], d1p.at[t, half_rows + 1], up
        return remote(src, dst, halo2_send.at[d, t], halo2_recv.at[d, t], to)

    for t in range(frames):
        halo1(0, t).start()
        halo1(1, t).start()

    for i in range(3):
        for j in range(3):
            w2_copy(i, j).start()
    for k in range(2, len(plain)):
        plain_copy(k).start()

    a1p[0:2] = jnp.zeros((2,) + a1p.shape[1:], BF16)
    a2p[0:2] = jnp.zeros((2,) + a2p.shape[1:], BF16)

    for i in range(3):
        for j in range(3):
            w1_copy(i, j).wait()

    def first_row(t, y):
        acc = None
        for i in range(3):
            term = jnp.dot(vp[t, y + i], w1[i], preferred_element_type=F32)
            acc = term if acc is None else acc + term
        a1p[t + 2, y] = side_sum(acc, c1, width).astype(BF16)

    def inner_rows(t, carry):
        video_copy(t).wait()
        for y in range(1, rows - 1):
            first_row(t, y)
        return carry

    lax.fori_loop(0, frames, inner_rows, 0)

    plain_copy(0).wait()
    plain_copy(1).wait()

    def first_level(t):
        halo1(0, t).wait_recv()
        halo1(1, t).wait_recv()

        @pl.when(ha == 0)
        def _():
            vp[t, 0] = jnp.zeros(vp.shape[2:], BF16)

        @pl.when(ha == n - 1)
        def _():
            vp[t, rows + 1] = jnp.zeros(vp.shape[2:], BF16)

        first_row(t, 0)
        first_row(t, rows - 1)
        for y in range(rows):
            stack = jnp.concatenate([a1p[t, y], a1p[t + 1, y], a1p[t + 2, y]], axis=1)
            h1s[y] = silu(jnp.dot(stack, t1v[...], preferred_element_type=F32))
        for y in range(half_rows):
            parts = [
                h1s[2 * y + i, pl.ds(j, half_width, stride=2), :].astype(BF16)
                for i in range(2)
                for j in range(2)
            ]
            d = jnp.dot(jnp.concatenate(parts, axis=1), r1v[...], preferred_element_type=F32)
            d1p[t, y + 1] = d.astype(BF16)
        halo2(0, t).start()
        halo2(1, t).start()

    for t in range(frames):
        first_level(t)

    for i in range(3):
        for j in range(3):
            w2_copy(i, j).wait()
    for k in (2, 3, 4):
        plain_copy(k).wait()

    def own_copy(t):
        return remote(
            keys.at[t, 0, 0, core], keys.at[t, 0, 0, core], own_send.at[t], own_recv.at[t], partner
        )

    def ring_copy(s, f):
        if isinstance(s, int) and s == 0:
            src, dst = keys.at[f, 0, 0], keys.at[f, 1, core]
        elif isinstance(s, int) and s == hops - 1:
            src, dst = keys.at[f, s, core], keys.at[f, 0, 1]
        else:
            src, dst = keys.at[f, s, core], keys.at[f, s + 1, core]
        return remote(
            src, dst, ring_send.at[lax.rem(s, 2), f], ring_recv.at[s + 1, f], after
        )

    def pair_copy(s, f):
        ref = keys.at[f, s, core]
        return remote(ref, ref, pair_send.at[lax.rem(s, 2), f], pair_recv.at[s, f], partner)

    def last_copy(f):
        ref = keys.at[f, 0, 1]
        return remote(ref, ref, last_send.at[lax.rem(f, half)], pair_recv.at[hops, f], partner)

    def second_level(t):
        halo2(0, t).wait_recv()
        halo2(1, t).wait_recv()

        @pl.when(ha == 0)
        def _():
            d1p[t, 0] = jnp.zeros(d1p.shape[2:], BF16)

        @pl.when(ha == n - 1)
        def _():
            d1p[t, half_rows + 1] = jnp.zeros(d1p.shape[2:], BF16)

        count = half_rows * half_width
        acc = None
        for i in range(3):
            block = d1p[t, i : i + half_rows].reshape(count, c2)
            term = jnp.dot(block, w2[i], preferred_element_type=F32)
            acc = term if acc is None else acc + term
        a2p[t + 2] = side_sum(acc, c2, half_width).astype(BF16)
        stack = jnp.concatenate([a2p[t], a2p[t + 1], a2p[t + 2]], axis=1)
        mid = silu(jnp.dot(stack, t2v[...], preferred_element_type=F32))
        mid = mid + d1p[t, 1 : half_rows + 1].reshape(count, c2).astype(F32)
        for b in range(c2 // 128):
            h2s[b] = mid[:, b * 128 : (b + 1) * 128]
        parts = [
            h2s[b, pl.ds(i * half_width + j, sites, stride=2), :].astype(BF16)
            for i in range(2)
            for j in range(2)
            for b in range(c2 // 128)
        ]
        h3 = jnp.dot(jnp.concatenate(parts, axis=1), r2v[...], preferred_element_type=F32)
        h3 = h3.astype(BF16).astype(F32)
        res[t] = h3
        mean_square = jnp.mean(h3 * h3, axis=-1, keepdims=True)
        normed = h3 * lax.rsqrt(mean_square + 1e-06) * gainv[...].astype(F32)
        keys[t, 0, 0, core] = normed.astype(BF16)
        own_copy(t).start()

        if t > 0:
            own_copy(t - 1).wait_recv()
            ring_copy(0, t - 1).start()

    for t in range(frames):
        second_level(t)

    own_copy(frames - 1).wait_recv()
    ring_copy(0, frames - 1).start()

    plain_copy(5).wait()
    plain_copy(6).wait()
    normed = keys[:, 0, 0, core].reshape(frames * sites, c3)
    queries = jnp.dot(normed, wqv[...], preferred_element_type=F32).astype(BF16)
    mapped = lax.dot_general(
        queries, wkv[...], (((1,), (1,)), ((), ())), preferred_element_type=F32
    )
    mapped = (mapped * (1.0 / math.sqrt(c3))).astype(BF16)
    qp[...] = mapped.reshape(frames, sites, c3)
    top[...] = jnp.full(top.shape, -1e30, F32)
    total[...] = jnp.zeros(total.shape, F32)
    mixed[...] = jnp.zeros(mixed.shape, F32)

    def attend(s, f):
        block = keys[f, s].reshape(4 * sites, c3)
        scores = lax.dot_general(
            qp[f], block, (((1,), (1,)), ((), ())), preferred_element_type=F32
        )
        old = top[f]
        new = jnp.maximum(old, jnp.max(scores, axis=-1, keepdims=True))
        decay = jnp.exp(old - new)
        weights = jnp.exp(scores - new[:, :1])
        total[f] = total[f] * decay + jnp.sum(weights, axis=-1, keepdims=True)
        mixed[f] = mixed[f] * decay[:, :1] + jnp.dot(
            weights.astype(BF16), block, preferred_element_type=F32
        )
        top[f] = new

    def hop(s, carry):
        for f in range(frames):
            receive_from = remote(
                keys.at[f, s, core],
                keys.at[f, s, core],
                ring_send.at[lax.rem(s, 2), f],
                ring_recv.at[s, f],
                after,
            )
            receive_from.wait_recv()

            @pl.when(s >= 2)
            def _():
                ring_copy(s - 2, f).wait_send()

            ring_copy(s, f).start()

            @pl.when(s >= 3)
            def _():
                pair_copy(s - 2, f).wait_send()

            pair_copy(s, f).start()

            @pl.when(s >= 2)
            def _():
                pair_copy(s - 1, f).wait_recv()
                attend(s - 1, f)

        return carry

    lax.fori_loop(1, hops - 1, hop, 0)

    end = hops - 1
    for f in range(frames):
        ring_copy(end - 1, f).wait_recv()
        ring_copy(end - 2, f).wait_send()

        @pl.when(core == f // half)
        def _():
            ring_copy(end, f).start()

        pair_copy(end - 2, f).wait_send()
        pair_copy(end, f).start()
        pair_copy(end - 1, f).wait_recv()
        attend(end - 1, f)

    for f in range(frames):
        @pl.when(core == f // half)
        def _():
            ring_copy(end, f).wait_recv()
            last_copy(f).start()

        pair_copy(end, f).wait_recv()
        attend(end, f)

    for k in (7, 8):
        plain_copy(k).wait()
    for f in range(frames):
        @pl.when(core != f // half)
        def _():
            last_copy(f).wait_recv()

        attend(0, f)

    mean = jnp.concatenate([mixed[f] / total[f][:, :1] for f in range(frames)], axis=0)
    values = jnp.dot(mean.astype(BF16), wvv[...], preferred_element_type=F32).astype(BF16)
    encoded = res[...].reshape(frames * sites, c3) + jnp.dot(
        values, wov[...], preferred_element_type=F32
    )
    out[...] = encoded.astype(BF16).reshape(out.shape)

    for t in range(frames):
        for d in range(2):
            halo1(d, t).wait_send()
            halo2(d, t).wait_send()
        own_copy(t).wait_send()
        ring_copy(end - 1, t).wait_send()
        pair_copy(end - 1, t).wait_send()
        pair_copy(end, t).wait_send()

        @pl.when(core == t // half)
        def _():
            ring_copy(end, t).wait_send()
            last_copy(t).wait_send()


def per_device(n, video, s1, t1, r1, s2, t2, r2, gain, wq, wk, wv, wo):
    frames, rows, width, c0 = video.shape
    c1, c2, c3 = t1.shape[1], t2.shape[1], wq.shape[0]
    half_rows, half_width = rows // 2, width // 2
    sites = (half_rows // 2) * (half_width // 2)
    hops = n // 4
    dma = pltpu.SemaphoreType.DMA
    scratch = [
        pltpu.VMEM((frames, rows + 2, width, c0), BF16),
        pltpu.VMEM((3, c0, 3 * c1), BF16),
        pltpu.VMEM((3 * c1, c1), BF16),
        pltpu.VMEM((4 * c1, c2), BF16),
        pltpu.VMEM((3, c2, 3 * c2), BF16),
        pltpu.VMEM((3 * c2, c2), BF16),
        pltpu.VMEM((4 * c2, c3), BF16),
        pltpu.VMEM((1, c3), BF16),
        pltpu.VMEM((c3, c3), BF16),
        pltpu.VMEM((c3, c3), BF16),
        pltpu.VMEM((c3, c3), BF16),
        pltpu.VMEM((c3, c3), BF16),
        pltpu.VMEM((frames + 2, rows, width, c1), BF16),
        pltpu.VMEM((rows, width, c1), F32),
        pltpu.VMEM((frames, half_rows + 2, half_width, c2), BF16),
        pltpu.VMEM((frames + 2, half_rows * half_width, c2), BF16),
        pltpu.VMEM((c2 // 128, half_rows * half_width, 128), F32),
        pltpu.VMEM((frames, sites, c3), F32),
        pltpu.VMEM((frames, hops, 2, 2, sites, c3), BF16),
        pltpu.VMEM((frames, sites, c3), BF16),
        pltpu.VMEM((frames, sites, 128), F32),
        pltpu.VMEM((frames, sites, 128), F32),
        pltpu.VMEM((frames, sites, c3), F32),
        dma((frames,)),
        dma((3, 3)),
        dma((3, 3)),
        dma((9,)),
        dma((2, frames)),
        dma((2, frames)),
        dma((2, frames)),
        dma((2, frames)),
        dma((frames,)),
        dma((frames,)),
        dma((2, frames)),
        dma((hops + 1, frames)),
        dma((2, frames)),
        dma((hops + 1, frames)),
        dma((frames // 2,)),
    ]
    out = pl.pallas_call(
        functools.partial(kernel, n),
        out_shape=jax.ShapeDtypeStruct((frames, half_rows // 2, half_width // 2, c3), BF16),
        in_specs=[pl.BlockSpec(memory_space=pl.ANY)] * 12,
        out_specs=pl.BlockSpec(memory_space=pltpu.VMEM),
        scratch_shapes=scratch,
        compiler_params=pltpu.CompilerParams(
            collective_id=0, has_side_effects=True, vmem_limit_bytes=60 * 1024 * 1024
        ),
        name="encoder",
    )(
        video,
        s1,
        t1.reshape(3 * c1, c1),
        r1.reshape(4 * c1, c2),
        s2,
        t2.reshape(3 * c2, c2),
        r2.reshape(4 * c2, c3),
        gain.reshape(1, c3),
        wq,
        wk,
        wv,
        wo,
    )
    return out


def solution(mesh):
    placed = (P("groups", "ha", None, None),) + (P(),) * 11
    return jax.shard_map(
        functools.partial(per_device, mesh.shape["ha"]),
        mesh=mesh,
        in_specs=placed,
        out_specs=P("groups", "ha", None, None),
        check_vma=False,
    )
```

```python
import functools
import math

import jax
import jax.numpy as jnp
from jax import lax
from jax.experimental import pallas as pl
from jax.experimental.pallas import tpu as pltpu
from jax.sharding import PartitionSpec as P

F32 = jnp.float32
BF16 = jnp.bfloat16


def silu(x):
    return x / (1.0 + jnp.exp(-x))


def side_sum(acc, width, period):
    rows = acc.shape[0]
    site = lax.rem(lax.broadcasted_iota(jnp.int32, (rows, width), 0), period)
    low = pltpu.roll(acc[:, :width], 1, 0)
    high = pltpu.roll(acc[:, 2 * width :], rows - 1, 0)
    low = jnp.where(site == 0, 0.0, low)
    high = jnp.where(site == period - 1, 0.0, high)
    return acc[:, width : 2 * width] + low + high


def kernel(
    n,
    video,
    s1,
    t1,
    r1,
    s2,
    t2,
    r2,
    gain,
    wq,
    wk,
    wv,
    wo,
    out,
    vp,
    w1,
    t1v,
    r1v,
    w2,
    t2v,
    r2v,
    gainv,
    wqv,
    wkv,
    wvv,
    wov,
    a1p,
    h1s,
    d1p,
    a2p,
    h2s,
    res,
    keys,
    qp,
    top,
    total,
    mixed,
    video_sem,
    w1_sem,
    w2_sem,
    weight_sem,
    halo1_send,
    halo1_recv,
    halo2_send,
    halo2_recv,
    own_send,
    own_recv,
    ring_send,
    ring_recv,
    pair_send,
    pair_recv,
    last_send,
):
    frames, rows, width, _ = video.shape
    c1 = t1.shape[1]
    c2 = t2.shape[1]
    c3 = wq.shape[0]
    half_rows, half_width = rows // 2, width // 2
    sites = out.shape[1] * out.shape[2]
    half = frames // 2
    hops = n // 4

    ha = lax.axis_index("ha")
    core = lax.rem(ha, 2)
    up = lax.rem(ha + n - 1, n)
    down = lax.rem(ha + 1, n)
    partner = ha + 1 - 2 * core
    after = lax.rem(ha + n + 2 - 4 * core, n)
    two_up = lax.rem(ha + n - 2, n)
    two_down = lax.rem(ha + 2, n)

    barrier = pltpu.get_barrier_semaphore()
    for other in (up, down, two_up, two_down):
        pl.semaphore_signal(
            barrier, inc=1, device_id={"ha": other}, device_id_type=pl.DeviceIdType.MESH
        )

    def video_copy(t):
        return pltpu.make_async_copy(video.at[t], vp.at[t, pl.ds(1, rows)], video_sem.at[t])

    def w1_copy(i, j):
        return pltpu.make_async_copy(
            s1.at[i, j], w1.at[i, :, pl.ds(j * c1, c1)], w1_sem.at[i, j]
        )

    def w2_copy(i, j):
        return pltpu.make_async_copy(
            s2.at[i, j], w2.at[i, :, pl.ds(j * c2, c2)], w2_sem.at[i, j]
        )

    plain = ((t1, t1v), (r1, r1v), (t2, t2v), (r2, r2v), (gain, gainv), (wq, wqv), (wk, wkv), (wv, wvv), (wo, wov))

    def plain_copy(k):
        return pltpu.make_async_copy(plain[k][0], plain[k][1], weight_sem.at[k])

    for t in range(frames):
        video_copy(t).start()
    for i in range(3):
        for j in range(3):
            w1_copy(i, j).start()
    for k in range(2):
        plain_copy(k).start()

    def remote(src, dst, send, recv, to):
        return pltpu.make_async_remote_copy(
            src_ref=src,
            dst_ref=dst,
            send_sem=send,
            recv_sem=recv,
            device_id={"ha": to},
            device_id_type=pl.DeviceIdType.MESH,
        )

    def halo1(d, t):
        if d == 0:
            src, dst, to = vp.at[t, rows], vp.at[t, 0], down
        else:
            src, dst, to = vp.at[t, 1], vp.at[t, rows + 1], up
        return remote(src, dst, halo1_send.at[d, t], halo1_recv.at[d, t], to)

    def halo2(d, t):
        if d == 0:
            src, dst, to = d1p.at[t, half_rows], d1p.at[t, 0], down
        else:
            src, dst, to = d1p.at[t, 1], d1p.at[t, half_rows + 1], up
        return remote(src, dst, halo2_send.at[d, t], halo2_recv.at[d, t], to)

    a1p[0:2] = jnp.zeros((2,) + a1p.shape[1:], BF16)
    a2p[0:2] = jnp.zeros((2,) + a2p.shape[1:], BF16)

    pl.semaphore_wait(barrier, 4)
    for t in range(frames):
        video_copy(t).wait()
        halo1(0, t).start()
        halo1(1, t).start()

    for i in range(3):
        for j in range(3):
            w2_copy(i, j).start()
    for k in range(2, len(plain)):
        plain_copy(k).start()

    for i in range(3):
        for j in range(3):
            w1_copy(i, j).wait()

    def first_row(t, y):
        acc = None
        for i in range(3):
            term = jnp.dot(vp[t, y + i], w1[i], preferred_element_type=F32)
            acc = term if acc is None else acc + term
        a1p[t + 2, y] = side_sum(acc, c1, width).astype(BF16)

    def inner_rows(t, carry):
        for y in range(1, rows - 1):
            first_row(t, y)
        return carry

    lax.fori_loop(0, frames, inner_rows, 0)

    plain_copy(0).wait()
    plain_copy(1).wait()

    def first_level(t):
        halo1(0, t).wait_recv()
        halo1(1, t).wait_recv()

        @pl.when(ha == 0)
        def _():
            vp[t, 0] = jnp.zeros(vp.shape[2:], BF16)

        @pl.when(ha == n - 1)
        def _():
            vp[t, rows + 1] = jnp.zeros(vp.shape[2:], BF16)

        first_row(t, 0)
        first_row(t, rows - 1)
        for y in range(rows):
            stack = jnp.concatenate([a1p[t, y], a1p[t + 1, y], a1p[t + 2, y]], axis=1)
            h1s[y] = silu(jnp.dot(stack, t1v[...], preferred_element_type=F32))
        for y in range(half_rows):
            parts = [
                h1s[2 * y + i, pl.ds(j, half_width, stride=2), :].astype(BF16)
                for i in range(2)
                for j in range(2)
            ]
            d = jnp.dot(jnp.concatenate(parts, axis=1), r1v[...], preferred_element_type=F32)
            d1p[t, y + 1] = d.astype(BF16)
        halo2(0, t).start()
        halo2(1, t).start()

    def own_copy(t):
        return remote(
            keys.at[t, 0, 0, core], keys.at[t, 0, 0, core], own_send.at[t], own_recv.at[t], partner
        )

    def ring_copy(s, f):
        if isinstance(s, int) and s == 0:
            src, dst = keys.at[f, 0, 0], keys.at[f, 1, core]
        elif isinstance(s, int) and s == hops - 1:
            src, dst = keys.at[f, s, core], keys.at[f, 0, 1]
        else:
            src, dst = keys.at[f, s, core], keys.at[f, s + 1, core]
        return remote(
            src, dst, ring_send.at[lax.rem(s, 2), f], ring_recv.at[s + 1, f], after
        )

    def pair_copy(s, f):
        ref = keys.at[f, s, core]
        return remote(ref, ref, pair_send.at[lax.rem(s, 2), f], pair_recv.at[s, f], partner)

    def last_copy(f):
        ref = keys.at[f, 0, 1]
        return remote(ref, ref, last_send.at[lax.rem(f, half)], pair_recv.at[hops, f], partner)

    def second_level(t):
        halo2(0, t).wait_recv()
        halo2(1, t).wait_recv()

        @pl.when(ha == 0)
        def _():
            d1p[t, 0] = jnp.zeros(d1p.shape[2:], BF16)

        @pl.when(ha == n - 1)
        def _():
            d1p[t, half_rows + 1] = jnp.zeros(d1p.shape[2:], BF16)

        count = half_rows * half_width
        acc = None
        for i in range(3):
            block = d1p[t, i : i + half_rows].reshape(count, c2)
            term = jnp.dot(block, w2[i], preferred_element_type=F32)
            acc = term if acc is None else acc + term
        a2p[t + 2] = side_sum(acc, c2, half_width).astype(BF16)
        stack = jnp.concatenate([a2p[t], a2p[t + 1], a2p[t + 2]], axis=1)
        mid = silu(jnp.dot(stack, t2v[...], preferred_element_type=F32))
        mid = mid + d1p[t, 1 : half_rows + 1].reshape(count, c2).astype(F32)
        for b in range(c2 // 128):
            h2s[b] = mid[:, b * 128 : (b + 1) * 128]
        parts = [
            h2s[b, pl.ds(i * half_width + j, sites, stride=2), :].astype(BF16)
            for i in range(2)
            for j in range(2)
            for b in range(c2 // 128)
        ]
        h3 = jnp.dot(jnp.concatenate(parts, axis=1), r2v[...], preferred_element_type=F32)
        h3 = h3.astype(BF16).astype(F32)
        res[t] = h3
        mean_square = jnp.mean(h3 * h3, axis=-1, keepdims=True)
        normed = h3 * lax.rsqrt(mean_square + 1e-06) * gainv[...].astype(F32).reshape(1, c3)
        keys[t, 0, 0, core] = normed.astype(BF16)
        own_copy(t).start()

    def take(s, f):
        block = keys.at[f, s, core]
        remote(
            block, block, ring_send.at[lax.rem(s, 2), f], ring_recv.at[s, f], after
        ).wait_recv()

        if not isinstance(s, int):
            ring_copy(s - 2, f).wait_send()
        ring_copy(s, f).start()
        if not isinstance(s, int):

            @pl.when(s >= 3)
            def _():
                pair_copy(s - 2, f).wait_send()

        pair_copy(s, f).start()

    def leave(t):
        own_copy(t).wait_recv()
        ring_copy(0, t).start()

    lead = min(2, frames - 1)
    for t in range(frames + lead):
        if t < frames:
            first_level(t)
        if t == lead:
            for i in range(3):
                for j in range(3):
                    w2_copy(i, j).wait()
            for k in (2, 3, 4):
                plain_copy(k).wait()
        if lead < t < frames:
            leave(t - lead - 1)
        if t == frames + lead - 1:
            take(1, 0)
        if t >= lead:
            second_level(t - lead)
        if t >= max(frames, lead + 1):
            leave(t - lead - 1)
    take(1, 1)
    leave(frames - 1)
    for f in range(2, frames - 1):
        take(1, f)

    plain_copy(5).wait()
    plain_copy(6).wait()
    normed = keys[:, 0, 0, core].reshape(frames * sites, c3)
    queries = jnp.dot(normed, wqv[...], preferred_element_type=F32).astype(BF16)
    mapped = lax.dot_general(
        queries, wkv[...], (((1,), (1,)), ((), ())), preferred_element_type=F32
    )
    mapped = (mapped * (1.0 / math.sqrt(c3))).astype(BF16)
    qp[...] = mapped.reshape(frames, sites, c3)
    take(1, frames - 1)
    top[...] = jnp.full(top.shape, -1e30, F32)
    total[...] = jnp.zeros(total.shape, F32)
    mixed[...] = jnp.zeros(mixed.shape, F32)

    def attend(s, f):
        block = keys[f, s].reshape(4 * sites, c3)
        scores = lax.dot_general(
            qp[f], block, (((1,), (1,)), ((), ())), preferred_element_type=F32
        )
        old = top[f]
        new = jnp.maximum(old, jnp.max(scores, axis=-1, keepdims=True))
        decay = jnp.exp(old - new)
        weights = jnp.exp(scores - new[:, :1])
        total[f] = total[f] * decay + jnp.sum(weights, axis=-1, keepdims=True)
        mixed[f] = mixed[f] * decay[:, :1] + jnp.dot(
            weights.astype(BF16), block, preferred_element_type=F32
        )
        top[f] = new

    def hop(s, carry):
        for f in range(frames):
            take(s, f)
            pair_copy(s - 1, f).wait_recv()
            attend(s - 1, f)
        return carry

    lax.fori_loop(2, hops - 1, hop, 0)

    end = hops - 1
    for f in range(frames):
        ring_copy(end - 1, f).wait_recv()
        ring_copy(end - 2, f).wait_send()

        @pl.when(core == f // half)
        def _():
            ring_copy(end, f).start()

        pair_copy(end - 2, f).wait_send()
        pair_copy(end, f).start()
        pair_copy(end - 1, f).wait_recv()
        attend(end - 1, f)

    for f in range(frames):
        @pl.when(core == f // half)
        def _():
            ring_copy(end, f).wait_recv()
            last_copy(f).start()

        pair_copy(end, f).wait_recv()
        attend(end, f)

    for k in (7, 8):
        plain_copy(k).wait()
    for f in range(frames):
        @pl.when(core != f // half)
        def _():
            last_copy(f).wait_recv()

        attend(0, f)

    mean = jnp.concatenate([mixed[f] / total[f][:, :1] for f in range(frames)], axis=0)
    values = jnp.dot(mean.astype(BF16), wvv[...], preferred_element_type=F32).astype(BF16)
    encoded = res[...].reshape(frames * sites, c3) + jnp.dot(
        values, wov[...], preferred_element_type=F32
    )
    out[...] = encoded.astype(BF16).reshape(out.shape)

    for t in range(frames):
        for d in range(2):
            halo1(d, t).wait_send()
            halo2(d, t).wait_send()
        own_copy(t).wait_send()
        ring_copy(end - 1, t).wait_send()
        pair_copy(end - 1, t).wait_send()
        pair_copy(end, t).wait_send()

        @pl.when(core == t // half)
        def _():
            ring_copy(end, t).wait_send()
            last_copy(t).wait_send()


def per_device(n, video, s1, t1, r1, s2, t2, r2, gain, wq, wk, wv, wo):
    frames, rows, width, c0 = video.shape
    c1, c2, c3 = t1.shape[1], t2.shape[1], wq.shape[0]
    half_rows, half_width = rows // 2, width // 2
    sites = (half_rows // 2) * (half_width // 2)
    hops = n // 4
    dma = pltpu.SemaphoreType.DMA
    scratch = [
        pltpu.VMEM((frames, rows + 2, width, c0), BF16),
        pltpu.VMEM((3, c0, 3 * c1), BF16),
        pltpu.VMEM((3 * c1, c1), BF16),
        pltpu.VMEM((4 * c1, c2), BF16),
        pltpu.VMEM((3, c2, 3 * c2), BF16),
        pltpu.VMEM((3 * c2, c2), BF16),
        pltpu.VMEM((4 * c2, c3), BF16),
        pltpu.VMEM((c3,), BF16),
        pltpu.VMEM((c3, c3), BF16),
        pltpu.VMEM((c3, c3), BF16),
        pltpu.VMEM((c3, c3), BF16),
        pltpu.VMEM((c3, c3), BF16),
        pltpu.VMEM((frames + 2, rows, width, c1), BF16),
        pltpu.VMEM((rows, width, c1), F32),
        pltpu.VMEM((frames, half_rows + 2, half_width, c2), BF16),
        pltpu.VMEM((frames + 2, half_rows * half_width, c2), BF16),
        pltpu.VMEM((c2 // 128, half_rows * half_width, 128), F32),
        pltpu.VMEM((frames, sites, c3), F32),
        pltpu.VMEM((frames, hops, 2, 2, sites, c3), BF16),
        pltpu.VMEM((frames, sites, c3), BF16),
        pltpu.VMEM((frames, sites, 128), F32),
        pltpu.VMEM((frames, sites, 128), F32),
        pltpu.VMEM((frames, sites, c3), F32),
        dma((frames,)),
        dma((3, 3)),
        dma((3, 3)),
        dma((9,)),
        dma((2, frames)),
        dma((2, frames)),
        dma((2, frames)),
        dma((2, frames)),
        dma((frames,)),
        dma((frames,)),
        dma((2, frames)),
        dma((hops + 1, frames)),
        dma((2, frames)),
        dma((hops + 1, frames)),
        dma((frames // 2,)),
    ]
    out = pl.pallas_call(
        functools.partial(kernel, n),
        out_shape=jax.ShapeDtypeStruct((frames, half_rows // 2, half_width // 2, c3), BF16),
        in_specs=[pl.BlockSpec(memory_space=pl.ANY)] * 12,
        out_specs=pl.BlockSpec(memory_space=pltpu.VMEM),
        scratch_shapes=scratch,
        compiler_params=pltpu.CompilerParams(
            collective_id=0, has_side_effects=True, vmem_limit_bytes=60 * 1024 * 1024
        ),
        name="encoder",
    )(
        video,
        s1,
        t1.reshape(3 * c1, c1),
        r1.reshape(4 * c1, c2),
        s2,
        t2.reshape(3 * c2, c2),
        r2.reshape(4 * c2, c3),
        gain,
        wq,
        wk,
        wv,
        wo,
    )
    return out


def solution(mesh):
    placed = (P("groups", "ha", None, None),) + (P(),) * 11
    return jax.shard_map(
        functools.partial(per_device, mesh.shape["ha"]),
        mesh=mesh,
        in_specs=placed,
        out_specs=P("groups", "ha", None, None),
        check_vma=False,
    )
```

```python
import functools
import math

import jax
import jax.numpy as jnp
from jax import lax
from jax.experimental import pallas as pl
from jax.experimental.pallas import tpu as pltpu
from jax.sharding import PartitionSpec as P

F32 = jnp.float32
BF16 = jnp.bfloat16


def silu(x):
    return x / (1.0 + jnp.exp(-x))


def side_sum(acc, width, period):
    rows = acc.shape[0]
    site = lax.rem(lax.broadcasted_iota(jnp.int32, (rows, width), 0), period)
    low = pltpu.roll(acc[:, :width], 1, 0)
    high = pltpu.roll(acc[:, 2 * width :], rows - 1, 0)
    low = jnp.where(site == 0, 0.0, low)
    high = jnp.where(site == period - 1, 0.0, high)
    return acc[:, width : 2 * width] + low + high


def kernel(
    n,
    video,
    s1,
    t1,
    r1,
    s2,
    t2,
    r2,
    gain,
    wq,
    wk,
    wv,
    wo,
    out,
    vp,
    w1,
    t1v,
    r1v,
    w2,
    t2v,
    r2v,
    gainv,
    wqv,
    wkv,
    wvv,
    wov,
    a1p,
    h1s,
    d1p,
    a2p,
    h2s,
    res,
    keys,
    qp,
    top,
    total,
    mixed,
    video_sem,
    w1_sem,
    w2_sem,
    weight_sem,
    halo1_send,
    halo1_recv,
    halo2_send,
    halo2_recv,
    own_send,
    own_recv,
    ring_send,
    ring_recv,
    pair_send,
    pair_recv,
    last_send,
):
    frames, rows, width, _ = video.shape
    c1 = t1.shape[1]
    c2 = t2.shape[1]
    c3 = wq.shape[0]
    half_rows, half_width = rows // 2, width // 2
    sites = out.shape[1] * out.shape[2]
    half = frames // 2
    hops = n // 4

    ha = lax.axis_index("ha")
    core = lax.rem(ha, 2)
    up = lax.rem(ha + n - 1, n)
    down = lax.rem(ha + 1, n)
    partner = ha + 1 - 2 * core
    after = lax.rem(ha + n + 2 - 4 * core, n)
    two_up = lax.rem(ha + n - 2, n)
    two_down = lax.rem(ha + 2, n)

    barrier = pltpu.get_barrier_semaphore()
    for other in (up, down, two_up, two_down):
        pl.semaphore_signal(
            barrier, inc=1, device_id={"ha": other}, device_id_type=pl.DeviceIdType.MESH
        )

    def video_copy(t):
        return pltpu.make_async_copy(video.at[t], vp.at[t, pl.ds(1, rows)], video_sem.at[t])

    def w1_copy(i, j):
        return pltpu.make_async_copy(
            s1.at[i, j], w1.at[i, :, pl.ds(j * c1, c1)], w1_sem.at[i, j]
        )

    def w2_copy(i, j):
        return pltpu.make_async_copy(
            s2.at[i, j], w2.at[i, :, pl.ds(j * c2, c2)], w2_sem.at[i, j]
        )

    plain = ((t1, t1v), (r1, r1v), (t2, t2v), (r2, r2v), (gain, gainv), (wq, wqv), (wk, wkv), (wv, wvv), (wo, wov))

    def plain_copy(k):
        return pltpu.make_async_copy(plain[k][0], plain[k][1], weight_sem.at[k])

    for t in range(frames):
        video_copy(t).start()
    for i in range(3):
        for j in range(3):
            w1_copy(i, j).start()
    for k in range(2):
        plain_copy(k).start()

    def remote(src, dst, send, recv, to):
        return pltpu.make_async_remote_copy(
            src_ref=src,
            dst_ref=dst,
            send_sem=send,
            recv_sem=recv,
            device_id={"ha": to},
            device_id_type=pl.DeviceIdType.MESH,
        )

    def halo1(d, t):
        if d == 0:
            src, dst, to = video.at[t, rows - 1], vp.at[t, 0], down
        else:
            src, dst, to = video.at[t, 0], vp.at[t, rows + 1], up
        return remote(src, dst, halo1_send.at[d, t], halo1_recv.at[d, t], to)

    def halo2(d, t):
        if d == 0:
            src, dst, to = d1p.at[t, half_rows], d1p.at[t, 0], down
        else:
            src, dst, to = d1p.at[t, 1], d1p.at[t, half_rows + 1], up
        return remote(src, dst, halo2_send.at[d, t], halo2_recv.at[d, t], to)

    a1p[0:2] = jnp.zeros((2,) + a1p.shape[1:], BF16)
    a2p[0:2] = jnp.zeros((2,) + a2p.shape[1:], BF16)

    pl.semaphore_wait(barrier, 4)
    for t in range(frames):
        halo1(0, t).start()
        halo1(1, t).start()
    for t in range(frames):
        video_copy(t).wait()

    for i in range(3):
        for j in range(3):
            w2_copy(i, j).start()
    for k in range(2, len(plain)):
        plain_copy(k).start()

    for i in range(3):
        for j in range(3):
            w1_copy(i, j).wait()

    def first_row(t, y):
        acc = None
        for i in range(3):
            term = jnp.dot(vp[t, y + i], w1[i], preferred_element_type=F32)
            acc = term if acc is None else acc + term
        a1p[t + 2, y] = side_sum(acc, c1, width).astype(BF16)

    def inner_rows(t, carry):
        for y in range(1, rows - 1):
            first_row(t, y)
        return carry

    lax.fori_loop(0, frames, inner_rows, 0)

    plain_copy(0).wait()
    plain_copy(1).wait()

    def first_level(t):
        halo1(0, t).wait_recv()
        halo1(1, t).wait_recv()

        @pl.when(ha == 0)
        def _():
            vp[t, 0] = jnp.zeros(vp.shape[2:], BF16)

        @pl.when(ha == n - 1)
        def _():
            vp[t, rows + 1] = jnp.zeros(vp.shape[2:], BF16)

        first_row(t, 0)
        first_row(t, rows - 1)
        for y in range(rows):
            stack = jnp.concatenate([a1p[t, y], a1p[t + 1, y], a1p[t + 2, y]], axis=1)
            h1s[y] = silu(jnp.dot(stack, t1v[...], preferred_element_type=F32))
        for y in range(half_rows):
            parts = [
                h1s[2 * y + i, pl.ds(j, half_width, stride=2), :].astype(BF16)
                for i in range(2)
                for j in range(2)
            ]
            d = jnp.dot(jnp.concatenate(parts, axis=1), r1v[...], preferred_element_type=F32)
            d1p[t, y + 1] = d.astype(BF16)
        halo2(0, t).start()
        halo2(1, t).start()

    def own_copy(t):
        return remote(
            keys.at[t, 0, 0, core], keys.at[t, 0, 0, core], own_send.at[t], own_recv.at[t], partner
        )

    def ring_copy(s, f):
        if isinstance(s, int) and s == 0:
            src, dst = keys.at[f, 0, 0], keys.at[f, 1, core]
        elif isinstance(s, int) and s == hops - 1:
            src, dst = keys.at[f, s, core], keys.at[f, 0, 1]
        else:
            src, dst = keys.at[f, s, core], keys.at[f, s + 1, core]
        return remote(
            src, dst, ring_send.at[lax.rem(s, 2), f], ring_recv.at[s + 1, f], after
        )

    def pair_copy(s, f):
        ref = keys.at[f, s, core]
        return remote(ref, ref, pair_send.at[lax.rem(s, 2), f], pair_recv.at[s, f], partner)

    def last_copy(f):
        ref = keys.at[f, 0, 1]
        return remote(ref, ref, last_send.at[lax.rem(f, half)], pair_recv.at[hops, f], partner)

    def second_level(t):
        halo2(0, t).wait_recv()
        halo2(1, t).wait_recv()

        @pl.when(ha == 0)
        def _():
            d1p[t, 0] = jnp.zeros(d1p.shape[2:], BF16)

        @pl.when(ha == n - 1)
        def _():
            d1p[t, half_rows + 1] = jnp.zeros(d1p.shape[2:], BF16)

        count = half_rows * half_width
        acc = None
        for i in range(3):
            block = d1p[t, i : i + half_rows].reshape(count, c2)
            term = jnp.dot(block, w2[i], preferred_element_type=F32)
            acc = term if acc is None else acc + term
        a2p[t + 2] = side_sum(acc, c2, half_width).astype(BF16)
        stack = jnp.concatenate([a2p[t], a2p[t + 1], a2p[t + 2]], axis=1)
        mid = silu(jnp.dot(stack, t2v[...], preferred_element_type=F32))
        mid = mid + d1p[t, 1 : half_rows + 1].reshape(count, c2).astype(F32)
        for b in range(c2 // 128):
            h2s[b] = mid[:, b * 128 : (b + 1) * 128]
        parts = [
            h2s[b, pl.ds(i * half_width + j, sites, stride=2), :].astype(BF16)
            for i in range(2)
            for j in range(2)
            for b in range(c2 // 128)
        ]
        h3 = jnp.dot(jnp.concatenate(parts, axis=1), r2v[...], preferred_element_type=F32)
        h3 = h3.astype(BF16).astype(F32)
        res[t] = h3
        mean_square = jnp.mean(h3 * h3, axis=-1, keepdims=True)
        normed = h3 * lax.rsqrt(mean_square + 1e-06) * gainv[...].astype(F32).reshape(1, c3)
        keys[t, 0, 0, core] = normed.astype(BF16)
        own_copy(t).start()

    def take(s, f):
        block = keys.at[f, s, core]
        remote(
            block, block, ring_send.at[lax.rem(s, 2), f], ring_recv.at[s, f], after
        ).wait_recv()

        if not isinstance(s, int):
            ring_copy(s - 2, f).wait_send()
        ring_copy(s, f).start()
        if not isinstance(s, int):

            @pl.when(s >= 3)
            def _():
                pair_copy(s - 2, f).wait_send()

        pair_copy(s, f).start()

    def leave(t):
        own_copy(t).wait_recv()
        ring_copy(0, t).start()

    for t in range(frames):
        first_level(t)
    for i in range(3):
        for j in range(3):
            w2_copy(i, j).wait()
    for k in (2, 3, 4):
        plain_copy(k).wait()
    for t in range(frames):
        second_level(t)
        if t > 0:
            leave(t - 1)
    leave(frames - 1)

    plain_copy(5).wait()
    plain_copy(6).wait()
    normed = keys[:, 0, 0, core].reshape(frames * sites, c3)
    queries = jnp.dot(normed, wqv[...], preferred_element_type=F32).astype(BF16)
    mapped = lax.dot_general(
        queries, wkv[...], (((1,), (1,)), ((), ())), preferred_element_type=F32
    )
    mapped = (mapped * (1.0 / math.sqrt(c3))).astype(BF16)
    qp[...] = mapped.reshape(frames, sites, c3)
    for f in range(frames):
        take(1, f)
    top[...] = jnp.full(top.shape, -1e30, F32)
    total[...] = jnp.zeros(total.shape, F32)
    mixed[...] = jnp.zeros(mixed.shape, F32)

    def attend(s, f):
        block = keys[f, s].reshape(4 * sites, c3)
        scores = lax.dot_general(
            qp[f], block, (((1,), (1,)), ((), ())), preferred_element_type=F32
        )
        old = top[f]
        new = jnp.maximum(old, jnp.max(scores, axis=-1, keepdims=True))
        decay = jnp.exp(old - new)
        weights = jnp.exp(scores - new[:, :1])
        total[f] = total[f] * decay + jnp.sum(weights, axis=-1, keepdims=True)
        mixed[f] = mixed[f] * decay[:, :1] + jnp.dot(
            weights.astype(BF16), block, preferred_element_type=F32
        )
        top[f] = new

    def hop(s, carry):
        for f in range(frames):
            take(s, f)
            pair_copy(s - 1, f).wait_recv()
            attend(s - 1, f)
        return carry

    lax.fori_loop(2, hops - 1, hop, 0)

    end = hops - 1
    for f in range(frames):
        ring_copy(end - 1, f).wait_recv()
        ring_copy(end - 2, f).wait_send()

        @pl.when(core == f // half)
        def _():
            ring_copy(end, f).start()

        pair_copy(end - 2, f).wait_send()
        pair_copy(end, f).start()
        pair_copy(end - 1, f).wait_recv()
        attend(end - 1, f)

    for f in range(frames):
        @pl.when(core == f // half)
        def _():
            ring_copy(end, f).wait_recv()
            last_copy(f).start()

        pair_copy(end, f).wait_recv()
        attend(end, f)

    for k in (7, 8):
        plain_copy(k).wait()
    for f in range(frames):
        @pl.when(core != f // half)
        def _():
            last_copy(f).wait_recv()

        attend(0, f)

    mean = jnp.concatenate([mixed[f] / total[f][:, :1] for f in range(frames)], axis=0)
    values = jnp.dot(mean.astype(BF16), wvv[...], preferred_element_type=F32).astype(BF16)
    encoded = res[...].reshape(frames * sites, c3) + jnp.dot(
        values, wov[...], preferred_element_type=F32
    )
    out[...] = encoded.astype(BF16).reshape(out.shape)

    for t in range(frames):
        for d in range(2):
            halo1(d, t).wait_send()
            halo2(d, t).wait_send()
        own_copy(t).wait_send()
        ring_copy(end - 1, t).wait_send()
        pair_copy(end - 1, t).wait_send()
        pair_copy(end, t).wait_send()

        @pl.when(core == t // half)
        def _():
            ring_copy(end, t).wait_send()
            last_copy(t).wait_send()


def per_device(n, video, s1, t1, r1, s2, t2, r2, gain, wq, wk, wv, wo):
    frames, rows, width, c0 = video.shape
    c1, c2, c3 = t1.shape[1], t2.shape[1], wq.shape[0]
    half_rows, half_width = rows // 2, width // 2
    sites = (half_rows // 2) * (half_width // 2)
    hops = n // 4
    dma = pltpu.SemaphoreType.DMA
    scratch = [
        pltpu.VMEM((frames, rows + 2, width, c0), BF16),
        pltpu.VMEM((3, c0, 3 * c1), BF16),
        pltpu.VMEM((3 * c1, c1), BF16),
        pltpu.VMEM((4 * c1, c2), BF16),
        pltpu.VMEM((3, c2, 3 * c2), BF16),
        pltpu.VMEM((3 * c2, c2), BF16),
        pltpu.VMEM((4 * c2, c3), BF16),
        pltpu.VMEM((c3,), BF16),
        pltpu.VMEM((c3, c3), BF16),
        pltpu.VMEM((c3, c3), BF16),
        pltpu.VMEM((c3, c3), BF16),
        pltpu.VMEM((c3, c3), BF16),
        pltpu.VMEM((frames + 2, rows, width, c1), BF16),
        pltpu.VMEM((rows, width, c1), F32),
        pltpu.VMEM((frames, half_rows + 2, half_width, c2), BF16),
        pltpu.VMEM((frames + 2, half_rows * half_width, c2), BF16),
        pltpu.VMEM((c2 // 128, half_rows * half_width, 128), F32),
        pltpu.VMEM((frames, sites, c3), F32),
        pltpu.VMEM((frames, hops, 2, 2, sites, c3), BF16),
        pltpu.VMEM((frames, sites, c3), BF16),
        pltpu.VMEM((frames, sites, 128), F32),
        pltpu.VMEM((frames, sites, 128), F32),
        pltpu.VMEM((frames, sites, c3), F32),
        dma((frames,)),
        dma((3, 3)),
        dma((3, 3)),
        dma((9,)),
        dma((2, frames)),
        dma((2, frames)),
        dma((2, frames)),
        dma((2, frames)),
        dma((frames,)),
        dma((frames,)),
        dma((2, frames)),
        dma((hops + 1, frames)),
        dma((2, frames)),
        dma((hops + 1, frames)),
        dma((frames // 2,)),
    ]
    out = pl.pallas_call(
        functools.partial(kernel, n),
        out_shape=jax.ShapeDtypeStruct((frames, half_rows // 2, half_width // 2, c3), BF16),
        in_specs=[pl.BlockSpec(memory_space=pl.ANY)] * 12,
        out_specs=pl.BlockSpec(memory_space=pltpu.VMEM),
        scratch_shapes=scratch,
        compiler_params=pltpu.CompilerParams(
            collective_id=0, has_side_effects=True, vmem_limit_bytes=60 * 1024 * 1024
        ),
        name="encoder",
    )(
        video,
        s1,
        t1.reshape(3 * c1, c1),
        r1.reshape(4 * c1, c2),
        s2,
        t2.reshape(3 * c2, c2),
        r2.reshape(4 * c2, c3),
        gain,
        wq,
        wk,
        wv,
        wo,
    )
    return out


def solution(mesh):
    placed = (P("groups", "ha", None, None),) + (P(),) * 11
    return jax.shard_map(
        functools.partial(per_device, mesh.shape["ha"]),
        mesh=mesh,
        in_specs=placed,
        out_specs=P("groups", "ha", None, None),
        check_vma=False,
    )
```

```python
import functools
import math

import jax
import jax.numpy as jnp
from jax import lax
from jax.experimental import pallas as pl
from jax.experimental.pallas import tpu as pltpu
from jax.sharding import PartitionSpec as P

F32 = jnp.float32
BF16 = jnp.bfloat16


def silu(x):
    return x / (1.0 + jnp.exp(-x))


def side_sum(acc, width, period):
    rows = acc.shape[0]
    site = lax.rem(lax.broadcasted_iota(jnp.int32, (rows, width), 0), period)
    low = pltpu.roll(acc[:, :width], 1, 0)
    high = pltpu.roll(acc[:, 2 * width :], rows - 1, 0)
    low = jnp.where(site == 0, 0.0, low)
    high = jnp.where(site == period - 1, 0.0, high)
    return acc[:, width : 2 * width] + low + high


def kernel(
    n,
    video,
    s1,
    t1,
    r1,
    s2,
    t2,
    r2,
    gain,
    wq,
    wk,
    wv,
    wo,
    out,
    vp,
    w1,
    t1v,
    r1v,
    w2,
    t2v,
    r2v,
    gainv,
    wqv,
    wkv,
    wvv,
    wov,
    a1p,
    h1s,
    d1p,
    a2p,
    h2s,
    res,
    keys,
    qp,
    top,
    total,
    mixed,
    video_sem,
    w1_sem,
    w2_sem,
    weight_sem,
    halo1_send,
    halo1_recv,
    halo2_send,
    halo2_recv,
    own_send,
    own_recv,
    ring_send,
    ring_recv,
    pair_send,
    pair_recv,
    last_send,
):
    frames, rows, width, _ = video.shape
    c1 = t1.shape[1]
    c2 = t2.shape[1]
    c3 = wq.shape[0]
    half_rows, half_width = rows // 2, width // 2
    sites = out.shape[1] * out.shape[2]
    half = frames // 2
    hops = n // 4

    ha = lax.axis_index("ha")
    core = lax.rem(ha, 2)
    up = lax.rem(ha + n - 1, n)
    down = lax.rem(ha + 1, n)
    partner = ha + 1 - 2 * core
    after = lax.rem(ha + n + 2 - 4 * core, n)
    two_up = lax.rem(ha + n - 2, n)
    two_down = lax.rem(ha + 2, n)

    barrier = pltpu.get_barrier_semaphore()
    for other in (up, down, two_up, two_down):
        pl.semaphore_signal(
            barrier, inc=1, device_id={"ha": other}, device_id_type=pl.DeviceIdType.MESH
        )

    def video_copy(t):
        return pltpu.make_async_copy(video.at[t], vp.at[t, pl.ds(1, rows)], video_sem.at[t])

    def w1_copy(i, j):
        return pltpu.make_async_copy(
            s1.at[i, j], w1.at[i, :, pl.ds(j * c1, c1)], w1_sem.at[i, j]
        )

    def w2_copy(i, j):
        return pltpu.make_async_copy(
            s2.at[i, j], w2.at[i, :, pl.ds(j * c2, c2)], w2_sem.at[i, j]
        )

    plain = ((t1, t1v), (r1, r1v), (t2, t2v), (r2, r2v), (gain, gainv), (wq, wqv), (wk, wkv), (wv, wvv), (wo, wov))

    def plain_copy(k):
        return pltpu.make_async_copy(plain[k][0], plain[k][1], weight_sem.at[k])

    for t in range(frames):
        video_copy(t).start()
    for i in range(3):
        for j in range(3):
            w1_copy(i, j).start()
    for k in range(2):
        plain_copy(k).start()

    def remote(src, dst, send, recv, to):
        return pltpu.make_async_remote_copy(
            src_ref=src,
            dst_ref=dst,
            send_sem=send,
            recv_sem=recv,
            device_id={"ha": to},
            device_id_type=pl.DeviceIdType.MESH,
        )

    def halo1(d, t):
        if d == 0:
            src, dst, to = video.at[t, rows - 1], vp.at[t, 0], down
        else:
            src, dst, to = video.at[t, 0], vp.at[t, rows + 1], up
        return remote(src, dst, halo1_send.at[d, t], halo1_recv.at[d, t], to)

    def halo2(d, t):
        if d == 0:
            src, dst, to = d1p.at[t, half_rows], d1p.at[t, 0], down
        else:
            src, dst, to = d1p.at[t, 1], d1p.at[t, half_rows + 1], up
        return remote(src, dst, halo2_send.at[d, t], halo2_recv.at[d, t], to)

    a1p[0:2] = jnp.zeros((2,) + a1p.shape[1:], BF16)
    a2p[0:2] = jnp.zeros((2,) + a2p.shape[1:], BF16)

    pl.semaphore_wait(barrier, 4)
    for t in range(frames):
        halo1(0, t).start()
        halo1(1, t).start()
    for t in range(frames):
        video_copy(t).wait()

    for i in range(3):
        for j in range(3):
            w2_copy(i, j).start()
    for k in range(2, len(plain)):
        plain_copy(k).start()

    for i in range(3):
        for j in range(3):
            w1_copy(i, j).wait()

    def first_row(t, y):
        acc = None
        for i in range(3):
            term = jnp.dot(vp[t, y + i], w1[i], preferred_element_type=F32)
            acc = term if acc is None else acc + term
        a1p[t + 2, y] = side_sum(acc, c1, width).astype(BF16)

    def inner_rows(t, carry):
        for y in range(1, rows - 1):
            first_row(t, y)
        return carry

    lax.fori_loop(0, frames, inner_rows, 0)

    plain_copy(0).wait()
    plain_copy(1).wait()

    def first_level(t):
        halo1(0, t).wait_recv()
        halo1(1, t).wait_recv()

        @pl.when(ha == 0)
        def _():
            vp[t, 0] = jnp.zeros(vp.shape[2:], BF16)

        @pl.when(ha == n - 1)
        def _():
            vp[t, rows + 1] = jnp.zeros(vp.shape[2:], BF16)

        first_row(t, 0)
        first_row(t, rows - 1)
        for y in range(rows):
            stack = jnp.concatenate([a1p[t, y], a1p[t + 1, y], a1p[t + 2, y]], axis=1)
            h1s[y] = silu(jnp.dot(stack, t1v[...], preferred_element_type=F32))
        for y in range(half_rows):
            parts = [
                h1s[2 * y + i, pl.ds(j, half_width, stride=2), :].astype(BF16)
                for i in range(2)
                for j in range(2)
            ]
            d = jnp.dot(jnp.concatenate(parts, axis=1), r1v[...], preferred_element_type=F32)
            d1p[t, y + 1] = d.astype(BF16)
        halo2(0, t).start()
        halo2(1, t).start()

    def own_copy(t):
        return remote(
            keys.at[t, 0, 0, core], keys.at[t, 0, 0, core], own_send.at[t], own_recv.at[t], partner
        )

    def ring_copy(s, f):
        if isinstance(s, int) and s == 0:
            src, dst = keys.at[f, 0, 0], keys.at[f, 1, core]
        elif isinstance(s, int) and s == hops - 1:
            src, dst = keys.at[f, s, core], keys.at[f, 0, 1]
        else:
            src, dst = keys.at[f, s, core], keys.at[f, s + 1, core]
        return remote(
            src, dst, ring_send.at[lax.rem(s, 2), f], ring_recv.at[s + 1, f], after
        )

    def pair_copy(s, f):
        ref = keys.at[f, s, core]
        return remote(ref, ref, pair_send.at[lax.rem(s, 2), f], pair_recv.at[s, f], partner)

    def last_copy(f):
        ref = keys.at[f, 0, 1]
        return remote(ref, ref, last_send.at[lax.rem(f, half)], pair_recv.at[hops, f], partner)

    def second_level(t):
        halo2(0, t).wait_recv()
        halo2(1, t).wait_recv()

        @pl.when(ha == 0)
        def _():
            d1p[t, 0] = jnp.zeros(d1p.shape[2:], BF16)

        @pl.when(ha == n - 1)
        def _():
            d1p[t, half_rows + 1] = jnp.zeros(d1p.shape[2:], BF16)

        count = half_rows * half_width
        acc = None
        for i in range(3):
            block = d1p[t, i : i + half_rows].reshape(count, c2)
            term = jnp.dot(block, w2[i], preferred_element_type=F32)
            acc = term if acc is None else acc + term
        a2p[t + 2] = side_sum(acc, c2, half_width).astype(BF16)
        stack = jnp.concatenate([a2p[t], a2p[t + 1], a2p[t + 2]], axis=1)
        mid = silu(jnp.dot(stack, t2v[...], preferred_element_type=F32))
        mid = mid + d1p[t, 1 : half_rows + 1].reshape(count, c2).astype(F32)
        for b in range(c2 // 128):
            h2s[b] = mid[:, b * 128 : (b + 1) * 128]
        parts = [
            h2s[b, pl.ds(i * half_width + j, sites, stride=2), :].astype(BF16)
            for i in range(2)
            for j in range(2)
            for b in range(c2 // 128)
        ]
        h3 = jnp.dot(jnp.concatenate(parts, axis=1), r2v[...], preferred_element_type=F32)
        h3 = h3.astype(BF16).astype(F32)
        res[t] = h3
        mean_square = jnp.mean(h3 * h3, axis=-1, keepdims=True)
        normed = h3 * lax.rsqrt(mean_square + 1e-06) * gainv[...].astype(F32).reshape(1, c3)
        keys[t, 0, 0, core] = normed.astype(BF16)
        own_copy(t).start()

    def take(s, f):
        block = keys.at[f, s, core]
        remote(
            block, block, ring_send.at[lax.rem(s, 2), f], ring_recv.at[s, f], after
        ).wait_recv()

        if not isinstance(s, int):
            ring_copy(s - 2, f).wait_send()
        ring_copy(s, f).start()
        if not isinstance(s, int):

            @pl.when(s >= 3)
            def _():
                pair_copy(s - 2, f).wait_send()

        pair_copy(s, f).start()

    def leave(t):
        own_copy(t).wait_recv()
        ring_copy(0, t).start()

    for t in range(frames):
        first_level(t)
    for i in range(3):
        for j in range(3):
            w2_copy(i, j).wait()
    for k in (2, 3, 4):
        plain_copy(k).wait()
    for t in range(frames):
        second_level(t)
        if t > 0:
            leave(t - 1)
    leave(frames - 1)

    plain_copy(5).wait()
    plain_copy(6).wait()
    normed = keys[:, 0, 0, core].reshape(frames * sites, c3)
    queries = jnp.dot(normed, wqv[...], preferred_element_type=F32).astype(BF16)
    mapped = lax.dot_general(
        queries, wkv[...], (((1,), (1,)), ((), ())), preferred_element_type=F32
    )
    mapped = (mapped * (1.0 / math.sqrt(c3))).astype(BF16)
    qp[...] = mapped.reshape(frames, sites, c3)
    for f in range(frames):
        take(1, f)
    top[...] = jnp.full(top.shape, -1e30, F32)
    total[...] = jnp.zeros(total.shape, F32)
    mixed[...] = jnp.zeros(mixed.shape, F32)

    def attend(s, f):
        block = keys[f, s].reshape(4 * sites, c3)
        scores = lax.dot_general(
            qp[f], block, (((1,), (1,)), ((), ())), preferred_element_type=F32
        )
        old = top[f]
        new = jnp.maximum(old, jnp.max(scores, axis=-1, keepdims=True))
        decay = jnp.exp(old - new)
        weights = jnp.exp(scores - new[:, :1])
        total[f] = total[f] * decay + jnp.sum(weights, axis=-1, keepdims=True)
        mixed[f] = mixed[f] * decay[:, :1] + jnp.dot(
            weights.astype(BF16), block, preferred_element_type=F32
        )
        top[f] = new

    def hop(s, carry):
        for f in range(frames):
            take(s, f)
            pair_copy(s - 1, f).wait_recv()
            attend(s - 1, f)
        return carry

    lax.fori_loop(2, hops - 1, hop, 0)

    end = hops - 1
    for f in range(frames):
        ring_copy(end - 1, f).wait_recv()
        ring_copy(end - 2, f).wait_send()

        @pl.when(core == f // half)
        def _():
            ring_copy(end, f).start()

        pair_copy(end - 2, f).wait_send()
        pair_copy(end, f).start()
        pair_copy(end - 1, f).wait_recv()
        attend(end - 1, f)

    def finish(group):
        mean = jnp.concatenate([mixed[f] / total[f][:, :1] for f in group], axis=0)
        values = jnp.dot(mean.astype(BF16), wvv[...], preferred_element_type=F32).astype(BF16)
        added = jnp.dot(values, wov[...], preferred_element_type=F32)
        for k, f in enumerate(group):
            encoded = res[f] + added[k * sites : (k + 1) * sites]
            out[f] = encoded.astype(BF16).reshape(out.shape[1:])

    for k in (7, 8):
        plain_copy(k).wait()
    groups = [(k, half + k) for k in range(half)]
    for k, group in enumerate(groups):
        for f in range(2 * k, 2 * k + 2):
            pair_copy(end, f).wait_recv()
        for f in range(2 * k, 2 * k + 2):
            attend(end, f)
        for f in group:

            @pl.when(core == f // half)
            def _():
                ring_copy(end, f).wait_recv()
                last_copy(f).start()

    for group in groups:
        for f in group:

            @pl.when(core != f // half)
            def _():
                last_copy(f).wait_recv()

        for f in group:
            attend(0, f)
        finish(group)

    for t in range(frames):
        for d in range(2):
            halo1(d, t).wait_send()
            halo2(d, t).wait_send()
        own_copy(t).wait_send()
        ring_copy(end - 1, t).wait_send()
        pair_copy(end - 1, t).wait_send()
        pair_copy(end, t).wait_send()

        @pl.when(core == t // half)
        def _():
            ring_copy(end, t).wait_send()
            last_copy(t).wait_send()


def per_device(n, video, s1, t1, r1, s2, t2, r2, gain, wq, wk, wv, wo):
    frames, rows, width, c0 = video.shape
    c1, c2, c3 = t1.shape[1], t2.shape[1], wq.shape[0]
    half_rows, half_width = rows // 2, width // 2
    sites = (half_rows // 2) * (half_width // 2)
    hops = n // 4
    dma = pltpu.SemaphoreType.DMA
    scratch = [
        pltpu.VMEM((frames, rows + 2, width, c0), BF16),
        pltpu.VMEM((3, c0, 3 * c1), BF16),
        pltpu.VMEM((3 * c1, c1), BF16),
        pltpu.VMEM((4 * c1, c2), BF16),
        pltpu.VMEM((3, c2, 3 * c2), BF16),
        pltpu.VMEM((3 * c2, c2), BF16),
        pltpu.VMEM((4 * c2, c3), BF16),
        pltpu.VMEM((c3,), BF16),
        pltpu.VMEM((c3, c3), BF16),
        pltpu.VMEM((c3, c3), BF16),
        pltpu.VMEM((c3, c3), BF16),
        pltpu.VMEM((c3, c3), BF16),
        pltpu.VMEM((frames + 2, rows, width, c1), BF16),
        pltpu.VMEM((rows, width, c1), F32),
        pltpu.VMEM((frames, half_rows + 2, half_width, c2), BF16),
        pltpu.VMEM((frames + 2, half_rows * half_width, c2), BF16),
        pltpu.VMEM((c2 // 128, half_rows * half_width, 128), F32),
        pltpu.VMEM((frames, sites, c3), F32),
        pltpu.VMEM((frames, hops, 2, 2, sites, c3), BF16),
        pltpu.VMEM((frames, sites, c3), BF16),
        pltpu.VMEM((frames, sites, 128), F32),
        pltpu.VMEM((frames, sites, 128), F32),
        pltpu.VMEM((frames, sites, c3), F32),
        dma((frames,)),
        dma((3, 3)),
        dma((3, 3)),
        dma((9,)),
        dma((2, frames)),
        dma((2, frames)),
        dma((2, frames)),
        dma((2, frames)),
        dma((frames,)),
        dma((frames,)),
        dma((2, frames)),
        dma((hops + 1, frames)),
        dma((2, frames)),
        dma((hops + 1, frames)),
        dma((frames // 2,)),
    ]
    out = pl.pallas_call(
        functools.partial(kernel, n),
        out_shape=jax.ShapeDtypeStruct((frames, half_rows // 2, half_width // 2, c3), BF16),
        in_specs=[pl.BlockSpec(memory_space=pl.ANY)] * 12,
        out_specs=pl.BlockSpec(memory_space=pltpu.VMEM),
        scratch_shapes=scratch,
        compiler_params=pltpu.CompilerParams(
            collective_id=0, has_side_effects=True, vmem_limit_bytes=60 * 1024 * 1024
        ),
        name="encoder",
    )(
        video,
        s1,
        t1.reshape(3 * c1, c1),
        r1.reshape(4 * c1, c2),
        s2,
        t2.reshape(3 * c2, c2),
        r2.reshape(4 * c2, c3),
        gain,
        wq,
        wk,
        wv,
        wo,
    )
    return out


def solution(mesh):
    placed = (P("groups", "ha", None, None),) + (P(),) * 11
    return jax.shard_map(
        functools.partial(per_device, mesh.shape["ha"]),
        mesh=mesh,
        in_specs=placed,
        out_specs=P("groups", "ha", None, None),
        check_vma=False,
    )
```

```python
import functools
import math

import jax
import jax.numpy as jnp
from jax import lax
from jax.experimental import pallas as pl
from jax.experimental.pallas import tpu as pltpu
from jax.sharding import PartitionSpec as P

F32 = jnp.float32
BF16 = jnp.bfloat16


def silu(x):
    return x / (1.0 + jnp.exp(-x))


def side_sum(acc, width, period):
    rows = acc.shape[0]
    site = lax.rem(lax.broadcasted_iota(jnp.int32, (rows, width), 0), period)
    low = pltpu.roll(acc[:, :width], 1, 0)
    high = pltpu.roll(acc[:, 2 * width :], rows - 1, 0)
    low = jnp.where(site == 0, 0.0, low)
    high = jnp.where(site == period - 1, 0.0, high)
    return acc[:, width : 2 * width] + low + high


def kernel(
    n,
    video,
    s1,
    t1,
    r1,
    s2,
    t2,
    r2,
    gain,
    wq,
    wk,
    wv,
    wo,
    out,
    vp,
    w1,
    t1v,
    r1v,
    w2,
    t2v,
    r2v,
    gainv,
    wqv,
    wkv,
    wvv,
    wov,
    a1p,
    h1s,
    d1p,
    a2p,
    h2s,
    res,
    keys,
    qp,
    top,
    total,
    mixed,
    video_sem,
    w1_sem,
    w2_sem,
    weight_sem,
    halo1_send,
    halo1_recv,
    halo2_send,
    halo2_recv,
    own_send,
    own_recv,
    ring_send,
    ring_recv,
    pair_send,
    pair_recv,
    last_send,
):
    frames, rows, width, _ = video.shape
    c1 = t1.shape[1]
    c2 = t2.shape[1]
    c3 = wq.shape[0]
    half_rows, half_width = rows // 2, width // 2
    sites = out.shape[1] * out.shape[2]
    half = frames // 2
    hops = n // 4

    ha = lax.axis_index("ha")
    core = lax.rem(ha, 2)
    up = lax.rem(ha + n - 1, n)
    down = lax.rem(ha + 1, n)
    partner = ha + 1 - 2 * core
    after = lax.rem(ha + n + 2 - 4 * core, n)
    two_up = lax.rem(ha + n - 2, n)
    two_down = lax.rem(ha + 2, n)

    barrier = pltpu.get_barrier_semaphore()
    for other in (up, down, two_up, two_down):
        pl.semaphore_signal(
            barrier, inc=1, device_id={"ha": other}, device_id_type=pl.DeviceIdType.MESH
        )

    def video_copy(t):
        return pltpu.make_async_copy(video.at[t], vp.at[t, pl.ds(1, rows)], video_sem.at[t])

    def w1_copy(i, j):
        return pltpu.make_async_copy(
            s1.at[i, j], w1.at[i, :, pl.ds(j * c1, c1)], w1_sem.at[i, j]
        )

    def w2_copy(i, j):
        return pltpu.make_async_copy(
            s2.at[i, j], w2.at[i, :, pl.ds(j * c2, c2)], w2_sem.at[i, j]
        )

    plain = ((t1, t1v), (r1, r1v), (t2, t2v), (r2, r2v), (gain, gainv), (wq, wqv), (wk, wkv), (wv, wvv), (wo, wov))

    def plain_copy(k):
        return pltpu.make_async_copy(plain[k][0], plain[k][1], weight_sem.at[k])

    for t in range(frames):
        video_copy(t).start()
    for i in range(3):
        for j in range(3):
            w1_copy(i, j).start()
    for k in range(2):
        plain_copy(k).start()

    def remote(src, dst, send, recv, to):
        return pltpu.make_async_remote_copy(
            src_ref=src,
            dst_ref=dst,
            send_sem=send,
            recv_sem=recv,
            device_id={"ha": to},
            device_id_type=pl.DeviceIdType.MESH,
        )

    def halo1(d, t):
        if d == 0:
            src, dst, to = video.at[t, rows - 1], vp.at[t, 0], down
        else:
            src, dst, to = video.at[t, 0], vp.at[t, rows + 1], up
        return remote(src, dst, halo1_send.at[d, t], halo1_recv.at[d, t], to)

    def halo2(d, t):
        if d == 0:
            src, dst, to = d1p.at[t, half_rows], d1p.at[t, 0], down
        else:
            src, dst, to = d1p.at[t, 1], d1p.at[t, half_rows + 1], up
        return remote(src, dst, halo2_send.at[d, t], halo2_recv.at[d, t], to)

    a1p[0:2] = jnp.zeros((2,) + a1p.shape[1:], BF16)
    a2p[0:2] = jnp.zeros((2,) + a2p.shape[1:], BF16)

    pl.semaphore_wait(barrier, 4)
    for t in range(frames):
        halo1(0, t).start()
        halo1(1, t).start()
    for t in range(frames):
        video_copy(t).wait()

    for i in range(3):
        for j in range(3):
            w2_copy(i, j).start()
    for k in range(2, len(plain)):
        plain_copy(k).start()

    for i in range(3):
        for j in range(3):
            w1_copy(i, j).wait()

    def first_row(t, y):
        acc = None
        for i in range(3):
            term = jnp.dot(vp[t, y + i], w1[i], preferred_element_type=F32)
            acc = term if acc is None else acc + term
        a1p[t + 2, y] = side_sum(acc, c1, width).astype(BF16)

    def inner_rows(t, carry):
        for y in range(1, rows - 1):
            first_row(t, y)
        return carry

    lax.fori_loop(0, frames, inner_rows, 0)

    plain_copy(0).wait()
    plain_copy(1).wait()

    def first_level(t):
        halo1(0, t).wait_recv()
        halo1(1, t).wait_recv()

        @pl.when(ha == 0)
        def _():
            vp[t, 0] = jnp.zeros(vp.shape[2:], BF16)

        @pl.when(ha == n - 1)
        def _():
            vp[t, rows + 1] = jnp.zeros(vp.shape[2:], BF16)

        first_row(t, 0)
        first_row(t, rows - 1)
        for y in range(rows):
            stack = jnp.concatenate([a1p[t, y], a1p[t + 1, y], a1p[t + 2, y]], axis=1)
            h1s[y] = silu(jnp.dot(stack, t1v[...], preferred_element_type=F32))
        for y in range(half_rows):
            parts = [
                h1s[2 * y + i, pl.ds(j, half_width, stride=2), :].astype(BF16)
                for i in range(2)
                for j in range(2)
            ]
            d = jnp.dot(jnp.concatenate(parts, axis=1), r1v[...], preferred_element_type=F32)
            d1p[t, y + 1] = d.astype(BF16)
        halo2(0, t).start()
        halo2(1, t).start()

    def own_copy(t):
        return remote(
            keys.at[t, 0, 0, core], keys.at[t, 0, 0, core], own_send.at[t], own_recv.at[t], partner
        )

    def ring_copy(s, f):
        if isinstance(s, int) and s == 0:
            src, dst = keys.at[f, 0, 0], keys.at[f, 1, core]
        elif isinstance(s, int) and s == hops - 1:
            src, dst = keys.at[f, s, core], keys.at[f, 0, 1]
        else:
            src, dst = keys.at[f, s, core], keys.at[f, s + 1, core]
        return remote(
            src, dst, ring_send.at[lax.rem(s, 2), f], ring_recv.at[s + 1, f], after
        )

    def pair_copy(s, f):
        ref = keys.at[f, s, core]
        return remote(ref, ref, pair_send.at[lax.rem(s, 2), f], pair_recv.at[s, f], partner)

    def last_copy(f):
        ref = keys.at[f, 0, 1]
        return remote(ref, ref, last_send.at[lax.rem(f, half)], pair_recv.at[hops, f], partner)

    def second_level(t):
        halo2(0, t).wait_recv()
        halo2(1, t).wait_recv()

        @pl.when(ha == 0)
        def _():
            d1p[t, 0] = jnp.zeros(d1p.shape[2:], BF16)

        @pl.when(ha == n - 1)
        def _():
            d1p[t, half_rows + 1] = jnp.zeros(d1p.shape[2:], BF16)

        count = half_rows * half_width
        acc = None
        for i in range(3):
            block = d1p[t, i : i + half_rows].reshape(count, c2)
            term = jnp.dot(block, w2[i], preferred_element_type=F32)
            acc = term if acc is None else acc + term
        a2p[t + 2] = side_sum(acc, c2, half_width).astype(BF16)
        stack = jnp.concatenate([a2p[t], a2p[t + 1], a2p[t + 2]], axis=1)
        mid = silu(jnp.dot(stack, t2v[...], preferred_element_type=F32))
        mid = mid + d1p[t, 1 : half_rows + 1].reshape(count, c2).astype(F32)
        for b in range(c2 // 128):
            h2s[b] = mid[:, b * 128 : (b + 1) * 128]
        parts = [
            h2s[b, pl.ds(i * half_width + j, sites, stride=2), :].astype(BF16)
            for i in range(2)
            for j in range(2)
            for b in range(c2 // 128)
        ]
        h3 = jnp.dot(jnp.concatenate(parts, axis=1), r2v[...], preferred_element_type=F32)
        h3 = h3.astype(BF16).astype(F32)
        res[t] = h3
        mean_square = jnp.mean(h3 * h3, axis=-1, keepdims=True)
        normed = h3 * lax.rsqrt(mean_square + 1e-06) * gainv[...].astype(F32).reshape(1, c3)
        keys[t, 0, 0, core] = normed.astype(BF16)
        own_copy(t).start()

    def take(s, f):
        block = keys.at[f, s, core]
        remote(
            block, block, ring_send.at[lax.rem(s, 2), f], ring_recv.at[s, f], after
        ).wait_recv()

        if not isinstance(s, int):
            ring_copy(s - 2, f).wait_send()
        ring_copy(s, f).start()
        if not isinstance(s, int):

            @pl.when(s >= 3)
            def _():
                pair_copy(s - 2, f).wait_send()

        pair_copy(s, f).start()

    def leave(t):
        own_copy(t).wait_recv()
        ring_copy(0, t).start()

    lead = min(2, frames - 1)
    for t in range(frames + lead):
        if t < frames:
            first_level(t)
        if t == lead:
            for i in range(3):
                for j in range(3):
                    w2_copy(i, j).wait()
            for k in (2, 3, 4):
                plain_copy(k).wait()
        if t >= lead:
            second_level(t - lead)
        if t > lead:
            leave(t - lead - 1)
    leave(frames - 1)

    plain_copy(5).wait()
    plain_copy(6).wait()
    normed = keys[:, 0, 0, core].reshape(frames * sites, c3)
    queries = jnp.dot(normed, wqv[...], preferred_element_type=F32).astype(BF16)
    mapped = lax.dot_general(
        queries, wkv[...], (((1,), (1,)), ((), ())), preferred_element_type=F32
    )
    mapped = (mapped * (1.0 / math.sqrt(c3))).astype(BF16)
    qp[...] = mapped.reshape(frames, sites, c3)
    for f in range(frames):
        take(1, f)
    top[...] = jnp.full(top.shape, -1e30, F32)
    total[...] = jnp.zeros(total.shape, F32)
    mixed[...] = jnp.zeros(mixed.shape, F32)

    def attend(s, f):
        block = keys[f, s].reshape(4 * sites, c3)
        scores = lax.dot_general(
            qp[f], block, (((1,), (1,)), ((), ())), preferred_element_type=F32
        )
        old = top[f]
        new = jnp.maximum(old, jnp.max(scores, axis=-1, keepdims=True))
        decay = jnp.exp(old - new)
        weights = jnp.exp(scores - new[:, :1])
        total[f] = total[f] * decay + jnp.sum(weights, axis=-1, keepdims=True)
        mixed[f] = mixed[f] * decay[:, :1] + jnp.dot(
            weights.astype(BF16), block, preferred_element_type=F32
        )
        top[f] = new

    def hop(s, carry):
        for f in range(frames):
            take(s, f)
            pair_copy(s - 1, f).wait_recv()
            attend(s - 1, f)
        return carry

    lax.fori_loop(2, hops - 1, hop, 0)

    end = hops - 1
    for f in range(frames):
        ring_copy(end - 1, f).wait_recv()
        ring_copy(end - 2, f).wait_send()

        @pl.when(core == f // half)
        def _():
            ring_copy(end, f).start()

        pair_copy(end - 2, f).wait_send()
        pair_copy(end, f).start()
        pair_copy(end - 1, f).wait_recv()
        attend(end - 1, f)

    def finish(group):
        mean = jnp.concatenate([mixed[f] / total[f][:, :1] for f in group], axis=0)
        values = jnp.dot(mean.astype(BF16), wvv[...], preferred_element_type=F32).astype(BF16)
        added = jnp.dot(values, wov[...], preferred_element_type=F32)
        for k, f in enumerate(group):
            encoded = res[f] + added[k * sites : (k + 1) * sites]
            out[f] = encoded.astype(BF16).reshape(out.shape[1:])

    for k in (7, 8):
        plain_copy(k).wait()
    groups = [(k, half + k) for k in range(half)]
    for k, group in enumerate(groups):
        for f in range(2 * k, 2 * k + 2):
            pair_copy(end, f).wait_recv()
        for f in range(2 * k, 2 * k + 2):
            attend(end, f)
        for f in group:

            @pl.when(core == f // half)
            def _():
                ring_copy(end, f).wait_recv()
                last_copy(f).start()

    for group in groups:
        for f in group:

            @pl.when(core != f // half)
            def _():
                last_copy(f).wait_recv()

        for f in group:
            attend(0, f)
        finish(group)

    for t in range(frames):
        for d in range(2):
            halo1(d, t).wait_send()
            halo2(d, t).wait_send()
        own_copy(t).wait_send()
        ring_copy(end - 1, t).wait_send()
        pair_copy(end - 1, t).wait_send()
        pair_copy(end, t).wait_send()

        @pl.when(core == t // half)
        def _():
            ring_copy(end, t).wait_send()
            last_copy(t).wait_send()


def per_device(n, video, s1, t1, r1, s2, t2, r2, gain, wq, wk, wv, wo):
    frames, rows, width, c0 = video.shape
    c1, c2, c3 = t1.shape[1], t2.shape[1], wq.shape[0]
    half_rows, half_width = rows // 2, width // 2
    sites = (half_rows // 2) * (half_width // 2)
    hops = n // 4
    dma = pltpu.SemaphoreType.DMA
    scratch = [
        pltpu.VMEM((frames, rows + 2, width, c0), BF16),
        pltpu.VMEM((3, c0, 3 * c1), BF16),
        pltpu.VMEM((3 * c1, c1), BF16),
        pltpu.VMEM((4 * c1, c2), BF16),
        pltpu.VMEM((3, c2, 3 * c2), BF16),
        pltpu.VMEM((3 * c2, c2), BF16),
        pltpu.VMEM((4 * c2, c3), BF16),
        pltpu.VMEM((c3,), BF16),
        pltpu.VMEM((c3, c3), BF16),
        pltpu.VMEM((c3, c3), BF16),
        pltpu.VMEM((c3, c3), BF16),
        pltpu.VMEM((c3, c3), BF16),
        pltpu.VMEM((frames + 2, rows, width, c1), BF16),
        pltpu.VMEM((rows, width, c1), F32),
        pltpu.VMEM((frames, half_rows + 2, half_width, c2), BF16),
        pltpu.VMEM((frames + 2, half_rows * half_width, c2), BF16),
        pltpu.VMEM((c2 // 128, half_rows * half_width, 128), F32),
        pltpu.VMEM((frames, sites, c3), F32),
        pltpu.VMEM((frames, hops, 2, 2, sites, c3), BF16),
        pltpu.VMEM((frames, sites, c3), BF16),
        pltpu.VMEM((frames, sites, 128), F32),
        pltpu.VMEM((frames, sites, 128), F32),
        pltpu.VMEM((frames, sites, c3), F32),
        dma((frames,)),
        dma((3, 3)),
        dma((3, 3)),
        dma((9,)),
        dma((2, frames)),
        dma((2, frames)),
        dma((2, frames)),
        dma((2, frames)),
        dma((frames,)),
        dma((frames,)),
        dma((2, frames)),
        dma((hops + 1, frames)),
        dma((2, frames)),
        dma((hops + 1, frames)),
        dma((frames // 2,)),
    ]
    out = pl.pallas_call(
        functools.partial(kernel, n),
        out_shape=jax.ShapeDtypeStruct((frames, half_rows // 2, half_width // 2, c3), BF16),
        in_specs=[pl.BlockSpec(memory_space=pl.ANY)] * 12,
        out_specs=pl.BlockSpec(memory_space=pltpu.VMEM),
        scratch_shapes=scratch,
        compiler_params=pltpu.CompilerParams(
            collective_id=0, has_side_effects=True, vmem_limit_bytes=60 * 1024 * 1024
        ),
        name="encoder",
    )(
        video,
        s1,
        t1.reshape(3 * c1, c1),
        r1.reshape(4 * c1, c2),
        s2,
        t2.reshape(3 * c2, c2),
        r2.reshape(4 * c2, c3),
        gain,
        wq,
        wk,
        wv,
        wo,
    )
    return out


def solution(mesh):
    placed = (P("groups", "ha", None, None),) + (P(),) * 11
    return jax.shard_map(
        functools.partial(per_device, mesh.shape["ha"]),
        mesh=mesh,
        in_specs=placed,
        out_specs=P("groups", "ha", None, None),
        check_vma=False,
    )
```
